32 devices in a mesh: dp: 32 (over z, y, x, core).
Axes of the slice: x: 2, y: 2, z: 4, core: 2. Of those that a mesh axis runs over, the one named last changes fastest.
Arguments:
- images: bfloat16 [128, 92, 4096], P('dp'), may hold values from -6 to 6
- layer_gain: float32 [4096], replicated, may hold values from 0.5 to 1.5
- in_weight: bfloat16 [4096, 1024], replicated, may hold values from -1 to 1
- out_weight: bfloat16 [1024, 1024], replicated, may hold values from -1 to 1
- text_embed: bfloat16 [128, 1024], P('dp'), may hold values from -6 to 6
- pair_index: int32 [128], P('dp'), may hold values from 0 to 127, each once
- logit_scale: float32 [1], replicated, may hold values from 30 to 200
Outputs:
- loss: float32 [1], replicated
- grad_norm: float32 [1], replicated
- update_image: float32 [128, 1024], P('dp')
- update_text: float32 [128, 1024], P('dp')
The draws below stay inside these ranges and needn't reach their ends.
Inputs may be any that keep to these rules, and one draw needn't show every extreme that they name: Image i is paired with text row pair_index[i]; every text row is paired with exactly one image.
All inputs are finite; a program needn't handle non-finite values.
Results may differ from the reference program's by a relative error of at most 0.0086.
Values may be sent and summed in bfloat16 or wider, within the bound.
No kernel may reach another device: no remote copies, remote signals or barrier semaphores. Data moves between devices by JAX's collectives and lax.ppermute only.
A program may use at most 64 MiB of HBM per device.

```python
import math
from functools import partial
import jax
import jax.numpy as jnp
from jax import lax

E = 1024
PS = 4096
TT = 92
B_DEV = 4
BATCH = 128


encoded_count = 64


rise_weight = 1.5


EPS_LAYER = 1e-05


def gain_values(key):
    noise = jax.random.normal(jax.random.fold_in(key, 301), (PS,), jnp.float32)
    return jnp.clip(1.0 + 0.1 * noise, 0.5, 1.5)


def input_matrix(key):
    noise = jax.random.normal(jax.random.fold_in(key, 303), (PS, E), jnp.float32)
    return jnp.clip(noise / math.sqrt(PS), -1.0, 1.0)


def output_matrix(key):
    noise = jax.random.normal(jax.random.fold_in(key, 305), (E, E), jnp.float32)
    return jnp.clip(noise / math.sqrt(E), -1.0, 1.0)


def draw_layer_gain(key, part):
    return gain_values(key)


def draw_in_weight(key, part):
    return input_matrix(key).astype(jnp.bfloat16)


def draw_out_weight(key, part):
    return output_matrix(key).astype(jnp.bfloat16)


def base_vector(key, row):
    return jax.random.normal(jax.random.fold_in(jax.random.fold_in(key, 101), row), (PS,), jnp.float32)


def token_noise(key, row):
    return jax.random.normal(jax.random.fold_in(jax.random.fold_in(key, 103), row), (TT, PS), jnp.float32)


def copied_row(key, row):
    device = row // B_DEV
    leader = jnp.where(device % 2 == 1, device * B_DEV, row)
    lead_base = base_vector(key, leader)
    lead_tokens = token_noise(key, leader)
    own_tokens = token_noise(key, row)
    extra = jnp.where(leader == row, 0.0, 0.01)
    mixed = 0.8 * lead_base[None, :] + 0.6 * lead_tokens + extra * own_tokens
    return jnp.clip(mixed, -6.0, 6.0).astype(jnp.bfloat16)


def draw_images(key, part):
    rows = jnp.arange(BATCH, dtype=jnp.int32)
    result = lax.map(lambda row: copied_row(key, row), rows)
    return result


def encode_images_drawn(pixels, layer_gain, in_weight, out_weight):
    values = pixels.astype(jnp.float32)
    average = jnp.mean(values, axis=-1, keepdims=True)
    centered = values - average
    variance = jnp.mean(centered * centered, axis=-1, keepdims=True)
    normed = (centered * lax.rsqrt(variance + EPS_LAYER) * layer_gain).astype(jnp.bfloat16)
    flattened = normed.reshape(-1, normed.shape[-1])
    hidden = jax.nn.gelu(jnp.dot(flattened, in_weight, preferred_element_type=jnp.float32), approximate=True)
    pooled = jnp.mean(hidden.reshape(pixels.shape[0], pixels.shape[1], -1), axis=1).astype(jnp.bfloat16)
    return jnp.dot(pooled, out_weight, preferred_element_type=jnp.float32)


def normalized(vector):
    return vector / jnp.sqrt(jnp.sum(vector * vector, axis=-1, keepdims=True))


def common_direction(key):
    rows = jnp.arange(encoded_count, dtype=jnp.int32)
    pixels = lax.map(lambda row: copied_row(key, row), rows)
    embedded = encode_images_drawn(pixels, gain_values(key), input_matrix(key).astype(jnp.bfloat16), output_matrix(key).astype(jnp.bfloat16))
    return normalized(jnp.mean(normalized(embedded), axis=0))


def rising_texts(key):
    noise = jax.random.normal(jax.random.fold_in(key, 231), (BATCH, E), jnp.float32)
    direction = common_direction(key)
    ranks = jnp.arange(BATCH, dtype=jnp.float32) / BATCH
    texts = noise - rise_weight * math.sqrt(E) * ranks[:, None] * direction[None, :]
    return jnp.clip(texts, -6.0, 6.0)


def draw_text_embed(key, part):
    texts = rising_texts(key)
    return texts.astype(jnp.bfloat16)


def draw_logit_scale(key, part):
    scale_key = jax.random.fold_in(key, 601)
    value = jnp.exp(jax.random.uniform(scale_key, (1,), jnp.float32, math.log(30.0), math.log(200.0)))
    return value


def setup_inputs(seed: int = 0) -> dict:
    key_list = jax.random.split(jax.random.key(seed), 8)
    images = draw_images(jax.random.fold_in(key_list[7], 71), 0)
    layer_gain = draw_layer_gain(jax.random.fold_in(key_list[7], 71), 0)
    in_weight = draw_in_weight(jax.random.fold_in(key_list[7], 71), 0)
    out_weight = draw_out_weight(jax.random.fold_in(key_list[7], 71), 0)
    text_embed = draw_text_embed(jax.random.fold_in(key_list[7], 71), 0)
    pair_index = jax.random.permutation(key_list[5], BATCH).astype(jnp.int32)
    logit_scale = draw_logit_scale(jax.random.fold_in(key_list[7], 71), 0)
    return dict(images=images, layer_gain=layer_gain, in_weight=in_weight, out_weight=out_weight, text_embed=text_embed, pair_index=pair_index, logit_scale=logit_scale)


EPS_UNIT = 1e-06
EPS_LAYER = 1e-05

def encode_images(pixels, layer_gain, in_weight, out_weight):
    values = pixels.astype(jnp.float32)
    average = lax.optimization_barrier(jnp.mean(values, axis=-1, keepdims=True))
    centered = values - average
    variance = lax.optimization_barrier(jnp.mean(centered * centered, axis=-1, keepdims=True))
    normed = (centered * lax.rsqrt(variance + EPS_LAYER) * layer_gain).astype(jnp.bfloat16)
    flattened = normed.reshape(-1, normed.shape[-1])
    hidden = jax.nn.gelu(jnp.dot(flattened, in_weight, preferred_element_type=jnp.float32), approximate=True)
    pooled = lax.optimization_barrier(jnp.mean(hidden.reshape(pixels.shape[0], pixels.shape[1], -1), axis=1)).astype(jnp.bfloat16)
    return jnp.dot(pooled, out_weight, preferred_element_type=jnp.float32)

def unit_rows(matrix):
    length = jnp.sqrt(lax.optimization_barrier(jnp.sum(matrix * matrix, axis=1, keepdims=True)) + EPS_UNIT)
    return (matrix / length, length)

def unit_backward(grad_unit, unit_vec, length):
    return (grad_unit - unit_vec * lax.optimization_barrier(jnp.sum(unit_vec * grad_unit, axis=1, keepdims=True))) / length

def reference(images, layer_gain, in_weight, out_weight, text_embed, pair_index, logit_scale):
    multiplier = logit_scale[0]
    blocks = images.reshape(BATCH // B_DEV, B_DEV, TT, PS)
    encoder = partial(encode_images, layer_gain=layer_gain, in_weight=in_weight, out_weight=out_weight)
    image_emb = lax.map(encoder, blocks).reshape(BATCH, -1)
    image_unit, image_len = unit_rows(image_emb)
    image_vec = image_unit.astype(jnp.bfloat16)
    text_unit, text_len = unit_rows(text_embed.astype(jnp.float32))
    text_vec = text_unit.astype(jnp.bfloat16)
    scores = multiplier * jnp.dot(image_vec, text_vec.T, preferred_element_type=jnp.float32)
    row_high = lax.optimization_barrier(jnp.max(scores, axis=1, keepdims=True))
    row_lse = row_high[:, 0] + jnp.log(lax.optimization_barrier(jnp.sum(jnp.exp(scores - row_high), axis=1)))
    col_high = lax.optimization_barrier(jnp.max(scores, axis=0, keepdims=True))
    col_lse = col_high[0, :] + jnp.log(lax.optimization_barrier(jnp.sum(jnp.exp(scores - col_high), axis=0)))
    target = jnp.arange(BATCH, dtype=jnp.int32)[None, :] == pair_index[:, None]
    positive = lax.optimization_barrier(jnp.sum(jnp.where(target, scores, jnp.zeros_like(scores)), axis=1))
    loss = (jnp.sum(row_lse) + jnp.sum(col_lse) - 2.0 * jnp.sum(positive)) / (2.0 * BATCH)
    weights = (jnp.exp(scores - row_lse[:, None]) + jnp.exp(scores - col_lse[None, :]) - 2.0 * target.astype(jnp.float32)).astype(jnp.bfloat16)
    grad_image_unit = multiplier * jnp.dot(weights, text_vec, preferred_element_type=jnp.float32)
    grad_text_unit = multiplier * jnp.dot(weights.T, image_vec, preferred_element_type=jnp.float32)
    grad_image = unit_backward(grad_image_unit, image_unit, image_len)
    grad_text = unit_backward(grad_text_unit, text_unit, text_len)
    squares = jnp.sum(grad_image * grad_image) + jnp.sum(grad_text * grad_text)
    factor = lax.rsqrt(squares / (2.0 * BATCH * E) + 1e-06)
    return (loss.reshape(1), jnp.sqrt(squares).reshape(1), grad_image * factor, grad_text * factor)
```

```python
import functools

import jax
import jax.numpy as jnp
from jax import lax
from jax.experimental import pallas as pl
from jax.experimental.pallas import tpu as pltpu
from jax.sharding import PartitionSpec as P

EPS_UNIT = 1e-06
EPS_LAYER = 1e-05
SIDE = 128
CHUNKS = 4


def exchange_phases(devices):
    bits = [1 << b for b in range(devices.bit_length() - 1)]
    phases = [[m] for m in reversed(bits[3:])]
    if len(bits) >= 3:
        phases.append([bits[1], bits[2], bits[1] | bits[2]])
    elif len(bits) == 2:
        phases.append([bits[1]])
    if bits:
        phases.append([bits[0]])
    return phases


def gather_relative(block, devices):
    for masks in exchange_phases(devices):
        parts = [block]
        for mask in masks:
            pairs = [(i, i ^ mask) for i in range(devices)]
            parts.append(lax.ppermute(block, "dp", pairs))
        block = jnp.concatenate(parts, axis=0)
    return block


def source_mask(slot, devices):
    result = jnp.zeros_like(slot)
    stride = 1
    for masks in exchange_phases(devices):
        count = len(masks) + 1
        digit = (slot // stride) % count
        for k, mask in enumerate(masks):
            result = jnp.where(digit == k + 1, result | mask, result)
        stride *= count
    return result


def encode_kernel(
    pair_ref, images_hbm, gain_ref, weight_hbm, text_ref, out_ref,
    images_ref, weight_ref, normed_ref, image_sems, weight_sems, *, group,
):
    tokens, local_rows, features = images_ref.shape
    width = weight_ref.shape[1]
    step = tokens // CHUNKS
    cols = width // CHUNKS

    def image_copy(c):
        part = pl.ds(c * step, step)
        return pltpu.make_async_copy(images_hbm.at[part], images_ref.at[part], image_sems.at[c])

    def weight_copy(c):
        part = pl.ds(c * cols, cols)
        return pltpu.make_async_copy(weight_hbm.at[:, part], weight_ref.at[:, part], weight_sems.at[c])

    for c in range(CHUNKS):
        image_copy(c).start()
    for c in range(CHUNKS):
        weight_copy(c).start()

    row = lax.broadcasted_iota(jnp.int32, (local_rows, SIDE), 0)
    lane = lax.broadcasted_iota(jnp.int32, (local_rows, SIDE), 1)
    pair = jnp.zeros((local_rows, SIDE), jnp.int32)
    for b in range(local_rows):
        pair = jnp.where(row == b, pair_ref[b], pair)
    digits = jnp.where(lane == 0, pair // 128, jnp.where(lane == 1, pair % 128, 0))
    out_ref[0, :, width : 2 * width] = text_ref[...]
    out_ref[0, :, 2 * width :] = digits.astype(jnp.float32).astype(jnp.bfloat16)

    rows = group * local_rows
    gain = gain_ref[...].reshape(1, features)

    def norm_group(g, carry):
        values = images_ref[pl.ds(g * group, group)].astype(jnp.float32).reshape(rows, features)
        average = jnp.sum(values, axis=1, keepdims=True) * (1.0 / features)
        centered = values - average
        variance = jnp.sum(centered * centered, axis=1, keepdims=True) * (1.0 / features)
        normed = centered * lax.rsqrt(variance + EPS_LAYER) * gain
        start = pl.multiple_of(g * rows, rows)
        normed_ref[pl.ds(start, rows), :] = normed.astype(jnp.bfloat16)
        return carry

    groups = tokens // group
    done = 0
    for c in range(CHUNKS):
        image_copy(c).wait()
        ready = ((c + 1) * step) // group
        lax.fori_loop(done, ready, norm_group, 0)
        done = ready
    for c in range(CHUNKS):
        weight_copy(c).wait()
        part = slice(c * cols, (c + 1) * cols)
        hidden = jax.nn.gelu(
            jnp.dot(normed_ref[...], weight_ref[:, part], preferred_element_type=jnp.float32),
            approximate=True,
        )
        folded = jnp.sum(hidden.reshape(-1, 2 * local_rows, cols), axis=0)
        total = folded[:local_rows] + folded[local_rows:]
        out_ref[0, :, part] = (total / tokens).astype(jnp.bfloat16)


def unit_rows(matrix):
    length = jnp.sqrt(jnp.sum(matrix * matrix, axis=1, keepdims=True) + EPS_UNIT)
    return (matrix / length, length)


def unit_backward(grad_unit, unit_vec, length):
    return (grad_unit - unit_vec * jnp.sum(unit_vec * grad_unit, axis=1, keepdims=True)) / length


def loss_kernel(
    device_ref, scale_ref, blocks_ref, weight_ref,
    loss_ref, norm_ref, image_out_ref, text_out_ref, image_grad_ref, text_grad_ref, *, devices,
):
    _, local_rows, packed = blocks_ref.shape
    width = weight_ref.shape[1]
    total_rows = devices * local_rows
    own = device_ref[0]
    multiplier = scale_ref[0]

    square = (total_rows, total_rows)
    row_ids = lax.broadcasted_iota(jnp.int32, square, 0)
    column_ids = lax.broadcasted_iota(jnp.int32, square, 1)
    slots = lax.broadcasted_iota(jnp.int32, (1, total_rows), 1)
    source = (source_mask(slots // local_rows, devices) ^ own) * local_rows + slots % local_rows
    order = (row_ids == source).astype(jnp.float32).astype(jnp.bfloat16)
    blocks = blocks_ref[...].reshape(total_rows, packed)
    ordered = jnp.dot(order, blocks, preferred_element_type=jnp.float32)

    text_unit, text_len = unit_rows(ordered[:, width : 2 * width])
    text_vec = text_unit.astype(jnp.bfloat16)
    pair = ordered[:, 2 * width : 2 * width + 1] * 128.0 + ordered[:, 2 * width + 1 : 2 * width + 2]
    target = column_ids == pair.astype(jnp.int32)
    pooled = ordered[:, :width].astype(jnp.bfloat16)
    image_unit, image_len = unit_rows(
        jnp.dot(pooled, weight_ref[...], preferred_element_type=jnp.float32)
    )
    image_vec = image_unit.astype(jnp.bfloat16)
    scores = multiplier * lax.dot_general(
        image_vec, text_vec, (((1,), (1,)), ((), ())), preferred_element_type=jnp.float32
    )
    row_high = jnp.max(scores, axis=1, keepdims=True)
    row_lse = row_high + jnp.log(jnp.sum(jnp.exp(scores - row_high), axis=1, keepdims=True))
    col_high = jnp.max(scores, axis=0, keepdims=True)
    col_lse = col_high + jnp.log(jnp.sum(jnp.exp(scores - col_high), axis=0, keepdims=True))
    positive = jnp.sum(jnp.where(target, scores, 0.0))
    loss = (jnp.sum(row_lse) + jnp.sum(col_lse) - 2.0 * positive) / (2.0 * total_rows)
    weights = (
        jnp.exp(scores - row_lse) + jnp.exp(scores - col_lse) - jnp.where(target, 2.0, 0.0)
    ).astype(jnp.bfloat16)
    grad_image_unit = multiplier * jnp.dot(weights, text_vec, preferred_element_type=jnp.float32)
    grad_text_unit = multiplier * lax.dot_general(
        weights, image_vec, (((0,), (0,)), ((), ())), preferred_element_type=jnp.float32
    )
    grad_image = unit_backward(grad_image_unit, image_unit, image_len)
    grad_text = unit_backward(grad_text_unit, text_unit, text_len)
    image_grad_ref[...] = grad_image.reshape(image_grad_ref.shape)
    text_grad_ref[...] = grad_text.reshape(text_grad_ref.shape)
    squares = jnp.sum(grad_image * grad_image + grad_text * grad_text, keepdims=True)
    factor = lax.rsqrt(squares / (2.0 * total_rows * width) + 1e-06)
    loss_ref[...] = jnp.full((1, 1), loss, jnp.float32)
    norm_ref[...] = jnp.sqrt(squares)
    image_out_ref[...] = image_grad_ref[own] * factor
    text_out_ref[...] = text_grad_ref[own] * factor


def per_device(images, layer_gain, in_weight, out_weight, text_embed, pair_index, logit_scale):
    local_rows, tokens, features = images.shape
    width = out_weight.shape[1]
    devices = lax.axis_size("dp")
    total_rows = devices * local_rows
    smem = pl.BlockSpec(memory_space=pltpu.SMEM)
    hbm = pl.BlockSpec(memory_space=pl.ANY)
    vmem = pl.BlockSpec(memory_space=pltpu.VMEM)
    packed = 2 * width + SIDE
    block = pl.pallas_call(
        functools.partial(encode_kernel, group=4),
        in_specs=[smem, hbm, vmem, hbm, vmem],
        out_specs=vmem,
        out_shape=jax.ShapeDtypeStruct((1, local_rows, packed), jnp.bfloat16),
        scratch_shapes=[
            pltpu.VMEM((tokens, local_rows, features), jnp.bfloat16),
            pltpu.VMEM(in_weight.shape, jnp.bfloat16),
            pltpu.VMEM((tokens * local_rows, features), jnp.bfloat16),
            pltpu.SemaphoreType.DMA((CHUNKS,)),
            pltpu.SemaphoreType.DMA((CHUNKS,)),
        ],
        name="encode",
    )(pair_index, images.transpose(1, 0, 2), layer_gain, in_weight, text_embed)
    blocks = gather_relative(block, devices)
    device = lax.axis_index("dp").astype(jnp.int32).reshape(1)
    loss, norm, update_image, update_text = pl.pallas_call(
        functools.partial(loss_kernel, devices=devices),
        in_specs=[smem, smem, vmem, vmem],
        out_specs=[vmem, vmem, vmem, vmem],
        out_shape=[
            jax.ShapeDtypeStruct((1, 1), jnp.float32),
            jax.ShapeDtypeStruct((1, 1), jnp.float32),
            jax.ShapeDtypeStruct((local_rows, width), jnp.float32),
            jax.ShapeDtypeStruct((local_rows, width), jnp.float32),
        ],
        scratch_shapes=[
            pltpu.VMEM((devices, local_rows, width), jnp.float32),
            pltpu.VMEM((devices, local_rows, width), jnp.float32),
        ],
        name="loss",
    )(device, logit_scale, blocks, out_weight)
    return (loss.reshape(1), norm.reshape(1), update_image, update_text)


def solution(mesh):
    placed = (P("dp", None, None), P(), P(), P(), P("dp", None), P("dp"), P())
    return jax.shard_map(
        per_device,
        mesh=mesh,
        in_specs=placed,
        out_specs=(P(), P(), P("dp", None), P("dp", None)),
        check_vma=False,
    )
```

```python
import functools

import jax
import jax.numpy as jnp
from jax import lax
from jax.experimental import pallas as pl
from jax.experimental.pallas import tpu as pltpu
from jax.sharding import PartitionSpec as P

EPS_UNIT = 1e-06
EPS_LAYER = 1e-05
SIDE = 128
CHUNKS = 4
VMEM_BYTES = 2 * 1024 * 1024


def exchange_phases(devices):
    bits = [1 << b for b in range(devices.bit_length() - 1)]
    phases = [[m] for m in reversed(bits[3:])]
    if len(bits) >= 3:
        phases.append([bits[1], bits[2], bits[1] | bits[2]])
    elif len(bits) == 2:
        phases.append([bits[1]])
    if bits:
        phases.append([bits[0]])
    return phases


def gather_relative(block, devices):
    for masks in exchange_phases(devices):
        parts = [block]
        for mask in masks:
            pairs = [(i, i ^ mask) for i in range(devices)]
            parts.append(lax.ppermute(block, "dp", pairs))
        block = jnp.concatenate(parts, axis=0)
    return block


def source_mask(slot, devices):
    result = jnp.zeros_like(slot)
    stride = 1
    for masks in exchange_phases(devices):
        count = len(masks) + 1
        digit = (slot // stride) % count
        for k, mask in enumerate(masks):
            result = jnp.where(digit == k + 1, result | mask, result)
        stride *= count
    return result


def encode_kernel(
    pair_ref, images_hbm, gain_ref, weight_hbm, text_ref, out_ref,
    images_ref, weight_ref, normed_ref, image_sems, weight_sems, *, group,
):
    tokens, local_rows, features = images_ref.shape
    width = weight_ref.shape[1]
    step = tokens // CHUNKS
    depth = features // CHUNKS

    def image_copy(c):
        part = pl.ds(c * step, step)
        return pltpu.make_async_copy(images_hbm.at[part], images_ref.at[part], image_sems.at[c])

    def weight_copy(c):
        part = pl.ds(c * depth, depth)
        return pltpu.make_async_copy(weight_hbm.at[part], weight_ref.at[part], weight_sems.at[c])

    for c in range(CHUNKS):
        image_copy(c).start()
    for c in range(CHUNKS):
        weight_copy(c).start()

    row = lax.broadcasted_iota(jnp.int32, (local_rows, SIDE), 0)
    lane = lax.broadcasted_iota(jnp.int32, (local_rows, SIDE), 1)
    pair = jnp.zeros((local_rows, SIDE), jnp.int32)
    for b in range(local_rows):
        pair = jnp.where(row == b, pair_ref[b], pair)
    digits = jnp.where(lane == 0, pair // 128, jnp.where(lane == 1, pair % 128, 0))
    out_ref[0, :, width : 2 * width] = text_ref[...]
    out_ref[0, :, 2 * width :] = digits.astype(jnp.float32).astype(jnp.bfloat16)

    rows = group * local_rows
    gain = gain_ref[...].reshape(1, features)

    def norm_group(g, carry):
        values = images_ref[pl.ds(g * group, group)].astype(jnp.float32).reshape(rows, features)
        average = jnp.sum(values, axis=1, keepdims=True) * (1.0 / features)
        centered = values - average
        variance = jnp.sum(centered * centered, axis=1, keepdims=True) * (1.0 / features)
        normed = centered * lax.rsqrt(variance + EPS_LAYER) * gain
        start = pl.multiple_of(g * rows, rows)
        normed_ref[pl.ds(start, rows), :] = normed.astype(jnp.bfloat16)
        return carry

    done = 0
    for c in range(CHUNKS):
        image_copy(c).wait()
        ready = ((c + 1) * step) // group
        lax.fori_loop(done, ready, norm_group, 0, unroll=2)
        done = ready
    for c in range(CHUNKS):
        weight_copy(c).wait()
    hidden = jax.nn.gelu(
        jnp.dot(normed_ref[...], weight_ref[...], preferred_element_type=jnp.float32),
        approximate=True,
    )
    folded = jnp.sum(hidden.reshape(-1, 2 * local_rows, width), axis=0)
    total = folded[:local_rows] + folded[local_rows:]
    out_ref[0, :, :width] = (total / tokens).astype(jnp.bfloat16)


def unit_rows(matrix):
    length = jnp.sqrt(jnp.sum(matrix * matrix, axis=1, keepdims=True) + EPS_UNIT)
    return (matrix / length, length)


def unit_backward(grad_unit, unit_vec, length):
    return (grad_unit - unit_vec * jnp.sum(unit_vec * grad_unit, axis=1, keepdims=True)) / length


def loss_kernel(
    device_ref, scale_ref, blocks_ref, weight_ref,
    loss_ref, norm_ref, image_out_ref, text_out_ref, image_grad_ref, text_grad_ref, *, devices,
):
    _, local_rows, packed = blocks_ref.shape
    width = weight_ref.shape[1]
    total_rows = devices * local_rows
    own = device_ref[0]
    multiplier = scale_ref[0]

    square = (total_rows, total_rows)
    row_ids = lax.broadcasted_iota(jnp.int32, square, 0)
    column_ids = lax.broadcasted_iota(jnp.int32, square, 1)
    slots = lax.broadcasted_iota(jnp.int32, (1, total_rows), 1)
    source = (source_mask(slots // local_rows, devices) ^ own) * local_rows + slots % local_rows
    order = (row_ids == source).astype(jnp.float32).astype(jnp.bfloat16)
    blocks = blocks_ref[...].reshape(total_rows, packed)
    ordered = jnp.dot(order, blocks, preferred_element_type=jnp.float32)

    text_unit, text_len = unit_rows(ordered[:, width : 2 * width])
    text_vec = text_unit.astype(jnp.bfloat16)
    pair = ordered[:, 2 * width : 2 * width + 1] * 128.0 + ordered[:, 2 * width + 1 : 2 * width + 2]
    target = column_ids == pair.astype(jnp.int32)
    pooled = ordered[:, :width].astype(jnp.bfloat16)
    image_unit, image_len = unit_rows(
        jnp.dot(pooled, weight_ref[...], preferred_element_type=jnp.float32)
    )
    image_vec = image_unit.astype(jnp.bfloat16)
    scores = multiplier * lax.dot_general(
        image_vec, text_vec, (((1,), (1,)), ((), ())), preferred_element_type=jnp.float32
    )
    row_high = jnp.max(scores, axis=1, keepdims=True)
    row_lse = row_high + jnp.log(jnp.sum(jnp.exp(scores - row_high), axis=1, keepdims=True))
    col_high = jnp.max(scores, axis=0, keepdims=True)
    col_lse = col_high + jnp.log(jnp.sum(jnp.exp(scores - col_high), axis=0, keepdims=True))
    positive = jnp.sum(jnp.where(target, scores, 0.0))
    loss = (jnp.sum(row_lse) + jnp.sum(col_lse) - 2.0 * positive) / (2.0 * total_rows)
    weights = (
        jnp.exp(scores - row_lse) + jnp.exp(scores - col_lse) - jnp.where(target, 2.0, 0.0)
    ).astype(jnp.bfloat16)
    grad_image_unit = multiplier * jnp.dot(weights, text_vec, preferred_element_type=jnp.float32)
    grad_text_unit = multiplier * lax.dot_general(
        weights, image_vec, (((0,), (0,)), ((), ())), preferred_element_type=jnp.float32
    )
    grad_image = unit_backward(grad_image_unit, image_unit, image_len)
    grad_text = unit_backward(grad_text_unit, text_unit, text_len)
    image_grad_ref[...] = grad_image.reshape(image_grad_ref.shape)
    text_grad_ref[...] = grad_text.reshape(text_grad_ref.shape)
    squares = jnp.sum(grad_image * grad_image + grad_text * grad_text, keepdims=True)
    factor = lax.rsqrt(squares / (2.0 * total_rows * width) + 1e-06)
    loss_ref[...] = jnp.full((1, 1), loss, jnp.float32)
    norm_ref[...] = jnp.sqrt(squares)
    image_out_ref[...] = image_grad_ref[own] * factor
    text_out_ref[...] = text_grad_ref[own] * factor


def in_vmem(array):
    if array.size * array.dtype.itemsize > VMEM_BYTES:
        return array
    return pltpu.with_memory_space_constraint(array, pltpu.VMEM)


def per_device(images, layer_gain, in_weight, out_weight, text_embed, pair_index, logit_scale):
    local_rows, tokens, features = images.shape
    width = out_weight.shape[1]
    devices = lax.axis_size("dp")
    total_rows = devices * local_rows
    smem = pl.BlockSpec(memory_space=pltpu.SMEM)
    hbm = pl.BlockSpec(memory_space=pl.ANY)
    vmem = pl.BlockSpec(memory_space=pltpu.VMEM)
    packed = 2 * width + SIDE
    block = pl.pallas_call(
        functools.partial(encode_kernel, group=4),
        in_specs=[smem, hbm, vmem, hbm, vmem],
        out_specs=vmem,
        out_shape=pltpu.VMEM((1, local_rows, packed), jnp.bfloat16),
        scratch_shapes=[
            pltpu.VMEM((tokens, local_rows, features), jnp.bfloat16),
            pltpu.VMEM(in_weight.shape, jnp.bfloat16),
            pltpu.VMEM((tokens * local_rows, features), jnp.bfloat16),
            pltpu.SemaphoreType.DMA((CHUNKS,)),
            pltpu.SemaphoreType.DMA((CHUNKS,)),
        ],
        name="encode",
    )(pair_index, images.transpose(1, 0, 2), layer_gain, in_weight, text_embed)
    blocks = gather_relative(block, devices)
    device = lax.axis_index("dp").astype(jnp.int32).reshape(1)
    loss, norm, update_image, update_text = pl.pallas_call(
        functools.partial(loss_kernel, devices=devices),
        in_specs=[smem, smem, vmem, vmem],
        out_specs=[vmem, vmem, vmem, vmem],
        out_shape=[
            jax.ShapeDtypeStruct((1, 1), jnp.float32),
            jax.ShapeDtypeStruct((1, 1), jnp.float32),
            jax.ShapeDtypeStruct((local_rows, width), jnp.float32),
            jax.ShapeDtypeStruct((local_rows, width), jnp.float32),
        ],
        scratch_shapes=[
            pltpu.VMEM((devices, local_rows, width), jnp.float32),
            pltpu.VMEM((devices, local_rows, width), jnp.float32),
        ],
        name="loss",
    )(device, logit_scale, in_vmem(blocks), in_vmem(out_weight))
    return (loss.reshape(1), norm.reshape(1), update_image, update_text)


def solution(mesh):
    placed = (P("dp", None, None), P(), P(), P(), P("dp", None), P("dp"), P())
    return jax.shard_map(
        per_device,
        mesh=mesh,
        in_specs=placed,
        out_specs=(P(), P(), P("dp", None), P("dp", None)),
        check_vma=False,
    )
```
